32 devices in a mesh: row: 8 (over z, y), col: 4 (over x, core).
Axes of the slice: x: 2, y: 2, z: 4, core: 2. Of those that a mesh axis runs over, the one named last changes fastest.
Arguments:
- right_side: float32 [8, 4, 8, 128], P('row', 'col'), may hold values from -6 to 6
- block_values: bfloat16 [8, 4, 8, 4, 128, 128], P('row', 'col'), may hold values from -0.25 to 0.25
- block_columns: int32 [8, 4, 8, 4], P('row', 'col'), may hold values from 0 to 71
- live_slots: int32 [8, 4, 8], P('row', 'col'), may hold values from 1 to 4
- row_scale: float32 [8, 4, 8, 128], P('row', 'col'), may hold values from 1 to 4
Outputs:
- solution_field: float32 [8, 4, 8, 128], P('row', 'col')
- hessenberg: float32 [5, 4], replicated
The draws below stay inside these ranges and needn't reach their ends.
Inputs may be any that keep to these rules, and one draw needn't show every extreme that they name: `block_columns`: an entry q names block q % 8 of the device at grid offset (q // 24 - 1, (q // 8) % 3 - 1); blocks outside the grid are zero. Only the first live_slots slots of a block row are used.
All inputs are finite; a program needn't handle non-finite values.
Results may differ from the reference program's by a relative error of at most 0.0012.
Values may be sent and summed in bfloat16 or wider, within the bound.
A program may use at most 64 MiB of HBM per device.

```python
import math
import jax
import jax.numpy as jnp
from jax import lax

NB = 8
BS = 128
SLOTS = 4
ITERS = 4
N_ROW = 8
N_COL = 4


def place_ends(drawn, rng, low, largest):
    longest = drawn.shape.index(max(drawn.shape))
    spots = []
    for shift in (0, 1):
        where = [jax.random.randint(jax.random.fold_in(rng, axis), (), 0, length) for axis, length in enumerate(drawn.shape)]
        where[longest] = (where[longest] + shift) % drawn.shape[longest]
        spots.append(tuple(where))
    return drawn.at[spots[0]].set(low).at[spots[1]].set(largest)


def block_scale(own_key, shape, split, least, top_value):
    gain = 1.0
    for axis_at, shards_of in split:
        heights = jax.random.uniform(jax.random.fold_in(jax.random.fold_in(own_key, 6), axis_at), (shards_of,), jnp.float32, least / len(split), top_value / len(split))
        gain = gain * jnp.repeat(jnp.exp(heights), shape[axis_at] // shards_of).reshape((-1,) + (1,) * (len(shape) - 1 - axis_at))
    return gain


def normal_values(stream_key, shape, spread, bound, split=(), kind=jnp.bfloat16):
    values = spread * jax.random.normal(stream_key, shape, jnp.float32)
    if split:
        values = values * block_scale(stream_key, shape, split, -0.22, 0.18)
    return jnp.clip(values, -bound, bound).astype(kind)


def setup_inputs(seed: int = 0) -> dict:
    keys = jax.random.split(jax.random.key(seed), 6)
    right_side = normal_values(keys[0], (N_ROW, N_COL, NB, BS), 1.0, 6.0, ((0, 8), (1, 4)), jnp.float32)
    block_values = normal_values(keys[1], (N_ROW, N_COL, NB, SLOTS, BS, BS), (BS * SLOTS) ** -0.5, 0.25, ((0, 8), (1, 4)))
    block_columns = place_ends(jax.random.randint(keys[2], (N_ROW, N_COL, NB, SLOTS), 0, 9 * NB), jax.random.fold_in(keys[2], 1), 0, (9 * NB) - 1).astype(jnp.int32)
    live_slots = place_ends(jax.random.randint(keys[3], (N_ROW, N_COL, NB), 1, SLOTS + 1), jax.random.fold_in(keys[3], 1), 1, SLOTS).astype(jnp.int32)
    row_scale = jnp.clip(jnp.exp(math.log(4.0) - 1.3862944 * jax.random.uniform(keys[4], (N_ROW, N_COL, NB, BS), jnp.float32) ** block_scale(keys[4], (N_ROW, N_COL, NB, BS), ((0, 8), (1, 4)), -0.2, 0.2)), 1.0, 4.0)
    return dict(right_side=right_side, block_values=block_values, block_columns=block_columns, live_slots=live_slots, row_scale=row_scale)


def neighbour_index(block_columns):
    row_count, col_count, block_count, slot_count = block_columns.shape
    grid_rows = jnp.arange(row_count, dtype=jnp.int32)[:, None, None, None]
    grid_cols = jnp.arange(col_count, dtype=jnp.int32)[None, :, None, None]
    offset_row = block_columns // (3 * block_count)
    offset_col = block_columns // block_count % 3
    within = block_columns % block_count
    return (((grid_rows + offset_row) * (col_count + 2) + grid_cols + offset_col) * block_count + within).astype(jnp.int32)

def operate(field, block_values, flat_index, live_mask, row_scale):
    rounded = field.astype(jnp.bfloat16)
    padded = jnp.pad(rounded, ((1, 1), (1, 1), (0, 0), (0, 0)))
    flat = padded.reshape(-1, rounded.shape[-1])
    picked = flat[flat_index] * live_mask

    def one_row(pair):
        values, pieces = pair
        return jnp.einsum('cnsij,cnsj->cni', values.astype(jnp.float32), pieces.astype(jnp.float32), precision=lax.Precision.HIGHEST)
    product = lax.map(one_row, (block_values, picked))
    return row_scale * field + product

def least_squares(hessenberg, initial_norm):
    gram = jnp.dot(hessenberg.T, hessenberg, precision=lax.Precision.HIGHEST)
    target = initial_norm * hessenberg[0, :]
    factor = jnp.linalg.cholesky(gram)
    steps_count = gram.shape[0]
    forward = []
    for ordinal in range(steps_count):
        accum = target[ordinal]
        for other in range(ordinal):
            accum = accum - factor[ordinal, other] * forward[other]
        forward.append(accum / factor[ordinal, ordinal])
    backward = [None] * steps_count
    for ordinal in reversed(range(steps_count)):
        accum = forward[ordinal]
        for other in range(ordinal + 1, steps_count):
            accum = accum - factor[other, ordinal] * backward[other]
        backward[ordinal] = accum / factor[ordinal, ordinal]
    return backward

def reference(right_side, block_values, block_columns, live_slots, row_scale):
    flat_index = neighbour_index(block_columns)
    slot_count = block_columns.shape[-1]
    live_mask = (jnp.arange(slot_count, dtype=jnp.int32)[None, None, None, :] < live_slots[..., None]).astype(jnp.bfloat16)[..., None]
    first_image = operate(right_side, block_values, flat_index, live_mask, row_scale)
    self_dot = jnp.sum(right_side * right_side)
    cross_dot = jnp.sum(right_side * first_image)
    image_dot = jnp.sum(first_image * first_image)
    initial_norm = jnp.sqrt(self_dot)
    basis = [right_side / initial_norm]
    residue = first_image / initial_norm
    projections = jnp.stack([cross_dot / self_dot])
    norm_square = image_dot / self_dot
    columns = []
    for iteration in range(ITERS):
        if iteration > 0:
            residue = operate(basis[-1], block_values, flat_index, live_mask, row_scale)
            projections = jnp.stack([jnp.sum(vector * residue) for vector in basis])
            norm_square = jnp.sum(residue * residue)
        height = jnp.sqrt(norm_square - jnp.sum(projections * projections))
        columns.append(jnp.concatenate([projections, height[None], jnp.zeros((ITERS - iteration - 1,), jnp.float32)]))
        if iteration + 1 < ITERS:
            for ordinal in range(len(basis)):
                residue = residue - projections[ordinal] * basis[ordinal]
            basis.append(residue / height)
    hessenberg = jnp.stack(columns, axis=1)
    weights = least_squares(hessenberg, initial_norm)
    solution_field = weights[0] * basis[0]
    for ordinal in range(1, ITERS):
        solution_field = solution_field + weights[ordinal] * basis[ordinal]
    return (solution_field, hessenberg)
```

```python
import functools

import jax
import jax.numpy as jnp
from jax import lax
from jax.experimental import pallas as pl
from jax.experimental.pallas import tpu as pltpu
from jax.sharding import PartitionSpec as P

ITERS = 4
MESH = pl.DeviceIdType.MESH
UNROLL_LIMIT = 64


def kernel(n_row, n_col, cols_ref, live_ref, rhs_hbm, scale_hbm, vals_hbm,
           field_ref, hess_ref,
           vals, scale, first, later, basis, dots, pieces, index,
           load_sem, vals_sem, halo_send, halo_recv, dot_send, dot_recv):
    f32 = jnp.float32
    row, col = lax.axis_index("row"), lax.axis_index("col")
    n_dev = n_row * n_col
    me = row * n_col + col
    blocks, slots, size = vals.shape[0], vals.shape[1], vals.shape[2]
    barrier = pltpu.get_barrier_semaphore()

    def field(stage):
        return first if stage == 0 else later.at[stage - 1]

    def part(stage, k):
        return field(stage).at[pl.ds(k * blocks, blocks)]

    load_rhs = pltpu.make_async_copy(rhs_hbm.at[0, 0], part(0, 4), load_sem.at[0])
    load_rhs.start()
    load_scale = pltpu.make_async_copy(scale_hbm.at[0, 0], scale, load_sem.at[1])
    load_scale.start()
    load_vals = [
        pltpu.make_async_copy(vals_hbm.at[0, 0, n], vals.at[n], vals_sem.at[n])
        for n in range(blocks)
    ]
    for copy in load_vals:
        copy.start()

    for stage in range(ITERS):
        for k in range(10):
            if k != 4:
                part(stage, k)[...] = jnp.zeros((blocks, size), f32)
    for n in range(blocks):
        for s in range(slots):
            index[n * slots + s] = jnp.where(
                s < live_ref[0, 0, n], cols_ref[0, 0, s, n], 9 * blocks)

    def others(act):
        if n_dev <= UNROLL_LIMIT:
            steps = sorted(range(1, n_dev), key=lambda t: abs(t - n_dev / 2))
            for t in steps:
                act((lax.rem(row + t // n_col, n_row), lax.rem(col + t % n_col, n_col)))
        else:
            def body(t, carry):
                act((lax.rem(row + t // n_col, n_row), lax.rem(col + t % n_col, n_col)))
                return carry
            lax.fori_loop(1, n_dev, body, 0)

    others(lambda where: pl.semaphore_signal(barrier, inc=1, device_id=where, device_id_type=MESH))
    pl.semaphore_wait(barrier, n_dev - 1)

    around = [(k, k // 3 - 1, k % 3 - 1) for k in range(9) if k != 4]

    def inside(a, b):
        ok = None
        for at, count, shift in ((row, n_row, a), (col, n_col, b)):
            if shift:
                here = (at > 0) if shift < 0 else (at < count - 1)
                ok = here if ok is None else jnp.logical_and(ok, here)
        return ok

    def halo_copy(stage, k, a, b):
        return pltpu.make_async_remote_copy(
            src_ref=part(stage, 4), dst_ref=part(stage, 8 - k),
            send_sem=halo_send.at[stage, k], recv_sem=halo_recv.at[stage, 8 - k],
            device_id=(row + a, col + b), device_id_type=MESH)

    def halo_start(stage):
        for k, a, b in around:
            @pl.when(inside(a, b))
            def _():
                halo_copy(stage, k, a, b).start()

    def halo_wait(stage):
        for k, a, b in around:
            @pl.when(inside(a, b))
            def _():
                pltpu.make_async_copy(
                    part(stage, k), part(stage, k), halo_recv.at[stage, k]).wait()

    def halo_done(stage):
        for k, a, b in around:
            @pl.when(inside(a, b))
            def _():
                pltpu.make_async_copy(
                    part(stage, 4), part(stage, 4), halo_send.at[stage, k]).wait()

    lane = lax.broadcasted_iota(jnp.int32, (1, size), 1)

    def reduce_start(stage, products):
        line = jnp.zeros((1, size), f32)
        for i, product in enumerate(products):
            line = jnp.where(lane == i, jnp.sum(product, keepdims=True), line)
        dots[stage, me] = line
        others(lambda where: pltpu.make_async_remote_copy(
            src_ref=dots.at[stage, me], dst_ref=dots.at[stage, me],
            send_sem=dot_send.at[stage], recv_sem=dot_recv.at[stage],
            device_id=where, device_id_type=MESH).start())

    def all_bytes(stage, sem):
        most = dots.at[stage, pl.ds(0, n_dev - 1)]
        return pltpu.make_async_copy(most, most, sem.at[stage])

    def reduce_wait(stage, count):
        all_bytes(stage, dot_recv).wait()
        if n_dev <= UNROLL_LIMIT:
            lines = [dots[stage, d] for d in range(n_dev)]
            while len(lines) > 1:
                lines = [sum(lines[i:i + 2]) for i in range(0, len(lines), 2)]
            total = lines[0]
        else:
            total = lax.fori_loop(
                0, n_dev, lambda d, acc: acc + dots[stage, d], jnp.zeros((1, size), f32))
        return [jnp.broadcast_to(total[:, i:i + 1], (blocks, size)) for i in range(count)]

    def operate(source, own):
        for n in range(blocks):
            for s in range(slots):
                pieces[n:n + 1, s * size:(s + 1) * size] = source[
                    pl.ds(index[n * slots + s], 1), :]
        left = pieces[...].astype(jnp.bfloat16)
        out = []
        for n in range(0, blocks, 2):
            acc = jnp.zeros((blocks, 2 * size), f32)
            for s in range(0, slots, 2):
                right = jnp.concatenate([
                    jnp.concatenate([vals[n + d, s], vals[n + d, s + 1]], axis=1)
                    for d in range(2)], axis=0)
                acc = acc + lax.dot_general(
                    left[:, s * size:(s + 2) * size], right,
                    (((1,), (1,)), ((), ())), preferred_element_type=f32)
            out.append(acc[n:n + 1, :size])
            out.append(acc[n + 1:n + 2, size:])
        return scale[...] * own + jnp.concatenate(out, axis=0)

    load_rhs.wait()
    halo_start(0)
    load_scale.wait()
    halo_wait(0)
    for copy in load_vals:
        copy.wait()
    own = pl.ds(4 * blocks, blocks)
    rhs = first[own, :]
    image = operate(first, rhs)
    later[0, own, :] = image
    reduce_start(0, [rhs * rhs, rhs * image, image * image])
    halo_start(1)

    def tall(x):
        return jnp.concatenate([x] * 10, axis=0)

    columns = []
    gram = [[None] * ITERS for _ in range(ITERS)]
    factor = [[None] * ITERS for _ in range(ITERS)]
    inverse = [None] * ITERS
    forward = []
    for j in range(ITERS):
        if j == 0:
            self_dot, cross_dot, image_dot = reduce_wait(0, 3)
            norm = jnp.sqrt(self_dot)
            inv_norm = 1.0 / norm
            inv_self = 1.0 / self_dot
            proj = [cross_dot * inv_self]
            square = image_dot * inv_self
        else:
            got = reduce_wait(j, j + 2)
            proj, square = got[:j + 1], got[j + 1]
        total = proj[0] * proj[0]
        for h in proj[1:]:
            total = total + h * h
        height = jnp.sqrt(square - total)
        if j + 1 < ITERS:
            halo_wait(j + 1)
            inv_height = 1.0 / height
            if j == 0:
                wide_norm = tall(inv_norm)
                basis[0] = first[...] * wide_norm
                w = later[0] * wide_norm
            else:
                w = later[j]
            for i in range(j + 1):
                w = w - tall(proj[i]) * basis[i]
            basis[j + 1] = w * tall(inv_height)
            here = [basis[i, own, :] for i in range(j + 2)]
            image = operate(basis.at[j + 1], here[-1])
            if j + 2 < ITERS:
                later[j + 1, own, :] = image
            reduce_start(j + 1, [v * image for v in here] + [image * image])
            if j + 2 < ITERS:
                halo_start(j + 2)
        columns.append(proj + [height])
        for i in range(j + 1):
            acc = columns[i][0] * columns[j][0]
            for m in range(1, i + 2):
                acc = acc + columns[i][m] * columns[j][m]
            gram[j][i] = acc
        for i in range(j + 1):
            acc = gram[j][i]
            for m in range(i):
                acc = acc - factor[j][m] * factor[i][m]
            if i == j:
                factor[j][j] = jnp.sqrt(acc)
                inverse[j] = 1.0 / factor[j][j]
            else:
                factor[j][i] = acc * inverse[i]
        acc = norm * columns[j][0]
        for m in range(j):
            acc = acc - factor[j][m] * forward[m]
        forward.append(acc * inverse[j])
    weights = [None] * ITERS
    for i in reversed(range(ITERS)):
        acc = forward[i]
        for m in range(i + 1, ITERS):
            acc = acc - factor[m][i] * weights[m]
        weights[i] = acc * inverse[i]
    result = weights[0] * basis[0, own, :]
    for i in range(1, ITERS):
        result = result + weights[i] * basis[i, own, :]
    field_ref[0, 0] = result
    down = lax.broadcasted_iota(jnp.int32, (blocks, size), 0)
    along = lax.broadcasted_iota(jnp.int32, (blocks, size), 1)
    hess = jnp.zeros((blocks, size), f32)
    for j in range(ITERS):
        for i in range(j + 2):
            hess = jnp.where((down == j) & (along == i), columns[j][i], hess)
    hess_ref[...] = hess[:ITERS, :ITERS + 1]
    for stage in range(ITERS):
        all_bytes(stage, dot_send).wait()
        halo_done(stage)


def on_device(right_side, block_values, block_columns, live_slots, row_scale):
    n_row, n_col = lax.axis_size("row"), lax.axis_size("col")
    blocks, slots, size = block_values.shape[2:5]
    f32 = jnp.float32
    result, hess = pl.pallas_call(
        functools.partial(kernel, n_row, n_col),
        out_shape=(
            jax.ShapeDtypeStruct(right_side.shape, f32),
            jax.ShapeDtypeStruct((ITERS, ITERS + 1), f32),
        ),
        in_specs=[pl.BlockSpec(memory_space=pltpu.SMEM)] * 2
        + [pl.BlockSpec(memory_space=pltpu.HBM)] * 3,
        out_specs=(pl.BlockSpec(memory_space=pltpu.VMEM),) * 2,
        scratch_shapes=[
            pltpu.VMEM((blocks, slots, size, size), jnp.bfloat16),
            pltpu.VMEM((blocks, size), f32),
            pltpu.VMEM((10 * blocks, size), f32),
            pltpu.VMEM((ITERS - 1, 10 * blocks, size), f32),
            pltpu.VMEM((ITERS, 10 * blocks, size), f32),
            pltpu.VMEM((ITERS, n_row * n_col, 1, size), f32),
            pltpu.VMEM((blocks, slots * size), f32),
            pltpu.SMEM((blocks * slots,), jnp.int32),
            pltpu.SemaphoreType.DMA((2,)),
            pltpu.SemaphoreType.DMA((blocks,)),
            pltpu.SemaphoreType.DMA((ITERS, 9)),
            pltpu.SemaphoreType.DMA((ITERS, 9)),
            pltpu.SemaphoreType.DMA((ITERS,)),
            pltpu.SemaphoreType.DMA((ITERS,)),
        ],
        compiler_params=pltpu.CompilerParams(
            collective_id=0, has_side_effects=True, vmem_limit_bytes=67_043_328),
    )(block_columns.swapaxes(2, 3), live_slots, right_side, row_scale, block_values)
    return result, hess.T


def solution(mesh):
    return jax.shard_map(
        on_device,
        mesh=mesh,
        in_specs=(
            P("row", "col", None, None),
            P("row", "col", None, None, None, None),
            P("row", "col", None, None),
            P("row", "col", None),
            P("row", "col", None, None),
        ),
        out_specs=(P("row", "col", None, None), P()),
        check_vma=False,
    )
```

```python
import functools

import jax
import jax.numpy as jnp
from jax import lax
from jax.experimental import pallas as pl
from jax.experimental.pallas import tpu as pltpu
from jax.sharding import PartitionSpec as P

ITERS = 4
MESH = pl.DeviceIdType.MESH
UNROLL_LIMIT = 64


def kernel(n_row, n_col, cols_ref, live_ref, rhs_hbm, scale_hbm, vals_hbm,
           field_ref, hess_ref,
           vals, scale, first, later, basis, dots, pieces, index,
           load_sem, vals_sem, halo_send, halo_recv, dot_send, dot_recv,
           meet_sem):
    f32 = jnp.float32
    row, col = lax.axis_index("row"), lax.axis_index("col")
    n_dev = n_row * n_col
    me = row * n_col + col
    blocks, slots, size = vals.shape[0], vals.shape[1], vals.shape[2]
    barrier = pltpu.get_barrier_semaphore()

    def field(stage):
        return first if stage == 0 else later.at[stage - 1]

    def part(stage, k):
        return field(stage).at[pl.ds(k * blocks, blocks)]

    load_rhs = pltpu.make_async_copy(rhs_hbm.at[0, 0], part(0, 4), load_sem.at[0])
    load_rhs.start()
    load_scale = pltpu.make_async_copy(scale_hbm.at[0, 0], scale, load_sem.at[1])
    load_scale.start()
    load_vals = [
        pltpu.make_async_copy(vals_hbm.at[0, 0, n], vals.at[n], vals_sem.at[n])
        for n in range(blocks)
    ]
    for copy in load_vals:
        copy.start()

    for stage in range(ITERS):
        for k in range(10):
            if k != 4:
                part(stage, k)[...] = jnp.zeros((blocks, size), f32)

    def others(act):
        if n_dev <= UNROLL_LIMIT:
            steps = sorted(range(1, n_dev), key=lambda t: abs(t - n_dev / 2))
            for t in steps:
                act((lax.rem(row + t // n_col, n_row), lax.rem(col + t % n_col, n_col)))
        else:
            def body(t, carry):
                act((lax.rem(row + t // n_col, n_row), lax.rem(col + t % n_col, n_col)))
                return carry
            lax.fori_loop(1, n_dev, body, 0)

    around = [(k, k // 3 - 1, k % 3 - 1) for k in range(9) if k != 4]

    def inside(a, b):
        ok = None
        for at, count, shift in ((row, n_row, a), (col, n_col, b)):
            if shift:
                here = (at >= -shift) if shift < 0 else (at < count - shift)
                ok = here if ok is None else jnp.logical_and(ok, here)
        return ok

    def greet(sem, reach):
        for _, a, b in around:
            @pl.when(inside(a * reach, b * reach))
            def _():
                pl.semaphore_signal(
                    sem, inc=1, device_id=(row + a * reach, col + b * reach),
                    device_id_type=MESH)

    def meet(sem, reach):
        count = 1
        for at, length in ((row, n_row), (col, n_col)):
            count = count * (1 + (at >= reach).astype(jnp.int32)
                             + (at < length - reach).astype(jnp.int32))
        pl.semaphore_wait(sem, count - 1)

    greet(barrier, 1)

    def halo_copy(stage, k, a, b):
        return pltpu.make_async_remote_copy(
            src_ref=part(stage, 4), dst_ref=part(stage, 8 - k),
            send_sem=halo_send.at[stage, k], recv_sem=halo_recv.at[stage, 8 - k],
            device_id=(row + a, col + b), device_id_type=MESH)

    def halo_start(stage):
        for k, a, b in around:
            @pl.when(inside(a, b))
            def _():
                halo_copy(stage, k, a, b).start()

    def halo_wait(stage):
        for k, a, b in around:
            @pl.when(inside(a, b))
            def _():
                pltpu.make_async_copy(
                    part(stage, k), part(stage, k), halo_recv.at[stage, k]).wait()

    def halo_done(stage):
        for k, a, b in around:
            @pl.when(inside(a, b))
            def _():
                pltpu.make_async_copy(
                    part(stage, 4), part(stage, 4), halo_send.at[stage, k]).wait()

    lane = lax.broadcasted_iota(jnp.int32, (1, size), 1)

    def reduce_start(stage, products):
        line = jnp.zeros((1, size), f32)
        for i, product in enumerate(products):
            line = jnp.where(lane == i, jnp.sum(product, keepdims=True), line)
        dots[stage, me] = line
        others(lambda where: pltpu.make_async_remote_copy(
            src_ref=dots.at[stage, me], dst_ref=dots.at[stage, me],
            send_sem=dot_send.at[stage], recv_sem=dot_recv.at[stage],
            device_id=where, device_id_type=MESH).start())

    def all_bytes(stage, sem):
        most = dots.at[stage, pl.ds(0, n_dev - 1)]
        return pltpu.make_async_copy(most, most, sem.at[stage])

    def reduce_wait(stage, count):
        all_bytes(stage, dot_recv).wait()
        if n_dev <= UNROLL_LIMIT:
            lines = [dots[stage, d] for d in range(n_dev)]
            while len(lines) > 1:
                lines = [sum(lines[i:i + 2]) for i in range(0, len(lines), 2)]
            total = lines[0]
        else:
            total = lax.fori_loop(
                0, n_dev, lambda d, acc: acc + dots[stage, d], jnp.zeros((1, size), f32))
        return [jnp.broadcast_to(total[:, i:i + 1], (blocks, size)) for i in range(count)]

    def operate(source, own):
        for n in range(blocks):
            for s in range(slots):
                pieces[n:n + 1, s * size:(s + 1) * size] = source[
                    pl.ds(index[n * slots + s], 1), :]
        left = pieces[...].astype(jnp.bfloat16)
        out = []
        for n in range(0, blocks, 2):
            acc = jnp.zeros((blocks, 2 * size), f32)
            for s in range(0, slots, 2):
                right = jnp.concatenate([
                    jnp.concatenate([vals[n + d, s], vals[n + d, s + 1]], axis=1)
                    for d in range(2)], axis=0)
                acc = acc + lax.dot_general(
                    left[:, s * size:(s + 2) * size], right,
                    (((1,), (1,)), ((), ())), preferred_element_type=f32)
            out.append(acc[n:n + 1, :size])
            out.append(acc[n + 1:n + 2, size:])
        return scale[...] * own + jnp.concatenate(out, axis=0)

    reaches = greetings(n_row, n_col)
    for n in range(blocks):
        for s in range(slots):
            index[n * slots + s] = jnp.where(
                s < live_ref[0, 0, n], cols_ref[0, 0, s, n], 9 * blocks)
    load_rhs.wait()
    meet(barrier, 1)
    halo_start(0)
    for i, reach in enumerate(reaches):
        greet(meet_sem.at[i], reach)
        if i + 1 < len(reaches):
            meet(meet_sem.at[i], reach)
    load_scale.wait()
    for copy in load_vals:
        copy.wait()
    halo_wait(0)
    own = pl.ds(4 * blocks, blocks)
    rhs = first[own, :]
    image = operate(first, rhs)
    later[0, own, :] = image
    if reaches:
        meet(meet_sem.at[len(reaches) - 1], reaches[-1])
    reduce_start(0, [rhs * rhs, rhs * image, image * image])
    halo_start(1)

    def tall(x):
        return jnp.concatenate([x] * 10, axis=0)

    columns = []
    gram = [[None] * ITERS for _ in range(ITERS)]
    factor = [[None] * ITERS for _ in range(ITERS)]
    inverse = [None] * ITERS
    forward = []
    for j in range(ITERS):
        if j == 0:
            self_dot, cross_dot, image_dot = reduce_wait(0, 3)
            norm = jnp.sqrt(self_dot)
            inv_norm = 1.0 / norm
            inv_self = 1.0 / self_dot
            proj = [cross_dot * inv_self]
            square = image_dot * inv_self
        else:
            got = reduce_wait(j, j + 2)
            proj, square = got[:j + 1], got[j + 1]
        total = proj[0] * proj[0]
        for h in proj[1:]:
            total = total + h * h
        height = jnp.sqrt(square - total)
        if j + 1 < ITERS:
            halo_wait(j + 1)
            inv_height = 1.0 / height
            if j == 0:
                wide_norm = tall(inv_norm)
                basis[0] = first[...] * wide_norm
                w = later[0] * wide_norm
            else:
                w = later[j]
            for i in range(j + 1):
                w = w - tall(proj[i]) * basis[i]
            basis[j + 1] = w * tall(inv_height)
            here = [basis[i, own, :] for i in range(j + 2)]
            image = operate(basis.at[j + 1], here[-1])
            if j + 2 < ITERS:
                later[j + 1, own, :] = image
            reduce_start(j + 1, [v * image for v in here] + [image * image])
            if j + 2 < ITERS:
                halo_start(j + 2)
        columns.append(proj + [height])
        for i in range(j + 1):
            acc = columns[i][0] * columns[j][0]
            for m in range(1, i + 2):
                acc = acc + columns[i][m] * columns[j][m]
            gram[j][i] = acc
        for i in range(j + 1):
            acc = gram[j][i]
            for m in range(i):
                acc = acc - factor[j][m] * factor[i][m]
            if i == j:
                factor[j][j] = jnp.sqrt(acc)
                inverse[j] = 1.0 / factor[j][j]
            else:
                factor[j][i] = acc * inverse[i]
        acc = norm * columns[j][0]
        for m in range(j):
            acc = acc - factor[j][m] * forward[m]
        forward.append(acc * inverse[j])
    weights = [None] * ITERS
    for i in reversed(range(ITERS)):
        acc = forward[i]
        for m in range(i + 1, ITERS):
            acc = acc - factor[m][i] * weights[m]
        weights[i] = acc * inverse[i]
    result = weights[0] * basis[0, own, :]
    for i in range(1, ITERS):
        result = result + weights[i] * basis[i, own, :]
    field_ref[0, 0] = result
    down = lax.broadcasted_iota(jnp.int32, (blocks, size), 0)
    along = lax.broadcasted_iota(jnp.int32, (blocks, size), 1)
    hess = jnp.zeros((blocks, size), f32)
    for j in range(ITERS):
        for i in range(j + 2):
            hess = jnp.where((down == j) & (along == i), columns[j][i], hess)
    hess_ref[...] = hess[:ITERS, :ITERS + 1]
    for stage in range(ITERS):
        all_bytes(stage, dot_send).wait()
        halo_done(stage)


def greetings(n_row, n_col):
    reaches, reach = [], 1
    while reach < max(n_row, n_col) - 1:
        reaches.append(reach)
        reach *= 2
    return reaches


def write_out(field_ref, hess_ref, field_out, hess_out, sems):
    copies = [
        pltpu.make_async_copy(field_ref, field_out, sems.at[0]),
        pltpu.make_async_copy(hess_ref, hess_out, sems.at[1]),
    ]
    for copy in copies:
        copy.start()
    for copy in copies:
        copy.wait()


def on_device(right_side, block_values, block_columns, live_slots, row_scale):
    n_row, n_col = lax.axis_size("row"), lax.axis_size("col")
    blocks, slots, size = block_values.shape[2:5]
    f32 = jnp.float32
    result, hess = pl.pallas_call(
        functools.partial(kernel, n_row, n_col),
        out_shape=(
            pltpu.VMEM(right_side.shape, f32),
            pltpu.VMEM((ITERS, ITERS + 1), f32),
        ),
        in_specs=[pl.BlockSpec(memory_space=pltpu.SMEM)] * 2
        + [pl.BlockSpec(memory_space=pltpu.HBM)] * 3,
        out_specs=(pl.BlockSpec(memory_space=pltpu.VMEM),) * 2,
        scratch_shapes=[
            pltpu.VMEM((blocks, slots, size, size), jnp.bfloat16),
            pltpu.VMEM((blocks, size), f32),
            pltpu.VMEM((10 * blocks, size), f32),
            pltpu.VMEM((ITERS - 1, 10 * blocks, size), f32),
            pltpu.VMEM((ITERS, 10 * blocks, size), f32),
            pltpu.VMEM((ITERS, n_row * n_col, 1, size), f32),
            pltpu.VMEM((blocks, slots * size), f32),
            pltpu.SMEM((blocks * slots,), jnp.int32),
            pltpu.SemaphoreType.DMA((2,)),
            pltpu.SemaphoreType.DMA((blocks,)),
            pltpu.SemaphoreType.DMA((ITERS, 9)),
            pltpu.SemaphoreType.DMA((ITERS, 9)),
            pltpu.SemaphoreType.DMA((ITERS,)),
            pltpu.SemaphoreType.DMA((ITERS,)),
            pltpu.SemaphoreType.REGULAR((max(1, len(greetings(n_row, n_col))),)),
        ],
        compiler_params=pltpu.CompilerParams(
            collective_id=0, has_side_effects=True, vmem_limit_bytes=60 << 20),
    )(block_columns.swapaxes(2, 3), live_slots, *[
        pltpu.with_memory_space_constraint(x, pltpu.HBM)
        for x in (right_side, row_scale, block_values)])
    result, hess = pl.pallas_call(
        write_out,
        out_shape=(
            jax.ShapeDtypeStruct(right_side.shape, f32),
            jax.ShapeDtypeStruct((ITERS, ITERS + 1), f32),
        ),
        in_specs=[pl.BlockSpec(memory_space=pltpu.VMEM)] * 2,
        out_specs=[pl.BlockSpec(memory_space=pltpu.HBM)] * 2,
        scratch_shapes=[pltpu.SemaphoreType.DMA((2,))],
        compiler_params=pltpu.CompilerParams(vmem_limit_bytes=1 << 20),
    )(result, hess)
    return result, hess.T


def solution(mesh):
    return jax.shard_map(
        on_device,
        mesh=mesh,
        in_specs=(
            P("row", "col", None, None),
            P("row", "col", None, None, None, None),
            P("row", "col", None, None),
            P("row", "col", None),
            P("row", "col", None, None),
        ),
        out_specs=(P("row", "col", None, None), P()),
        check_vma=False,
    )
```

```python
import functools

import jax
import jax.numpy as jnp
from jax import lax
from jax.experimental import pallas as pl
from jax.experimental.pallas import tpu as pltpu
from jax.sharding import PartitionSpec as P

ITERS = 4
MESH = pl.DeviceIdType.MESH
UNROLL_LIMIT = 64
REACH = 2


def kernel(n_row, n_col, cols_ref, live_ref, rhs_hbm, scale_hbm, vals_hbm,
           field_ref, hess_ref,
           vals, scale, first, later, basis, dots, pieces, index,
           load_sem, vals_sem, halo_send, halo_recv, dot_send, dot_recv,
           meet_sem):
    f32 = jnp.float32
    row, col = lax.axis_index("row"), lax.axis_index("col")
    n_dev = n_row * n_col
    me = row * n_col + col
    blocks, slots, size = vals.shape[0], vals.shape[1], vals.shape[2]
    barrier = pltpu.get_barrier_semaphore()

    def field(stage):
        return first if stage == 0 else later.at[stage - 1]

    def part(stage, k):
        return field(stage).at[pl.ds(k * blocks, blocks)]

    load_rhs = pltpu.make_async_copy(rhs_hbm.at[0, 0], part(0, 4), load_sem.at[0])
    load_rhs.start()
    load_scale = pltpu.make_async_copy(scale_hbm.at[0, 0], scale, load_sem.at[1])
    load_scale.start()
    load_vals = [
        pltpu.make_async_copy(vals_hbm.at[0, 0, n], vals.at[n], vals_sem.at[n])
        for n in range(blocks)
    ]
    for copy in load_vals:
        copy.start()

    for stage in range(ITERS):
        for k in range(10):
            if k != 4:
                part(stage, k)[...] = jnp.zeros((blocks, size), f32)

    def others(act):
        if n_dev <= UNROLL_LIMIT:
            steps = sorted(range(1, n_dev), key=lambda t: abs(t - n_dev / 2))
            for t in steps:
                act((lax.rem(row + t // n_col, n_row), lax.rem(col + t % n_col, n_col)))
        else:
            def body(t, carry):
                act((lax.rem(row + t // n_col, n_row), lax.rem(col + t % n_col, n_col)))
                return carry
            lax.fori_loop(1, n_dev, body, 0)

    around = [(k, k // 3 - 1, k % 3 - 1) for k in range(9) if k != 4]

    def inside(a, b):
        ok = None
        for at, count, shift in ((row, n_row, a), (col, n_col, b)):
            if shift:
                here = (at >= -shift) if shift < 0 else (at < count - shift)
                ok = here if ok is None else jnp.logical_and(ok, here)
        return ok

    def welcome():
        for a in range(-REACH, REACH + 1):
            def send(a=a):
                for c in range(1 if a == 0 else 0, n_col):
                    pl.semaphore_signal(
                        barrier, inc=1, device_id=(row + a, lax.rem(col + c, n_col)),
                        device_id_type=MESH)
            if a == 0:
                send()
            else:
                pl.when(inside(a, 0))(send)

    def rows_at(reach):
        return (row >= reach).astype(jnp.int32) + (row < n_row - reach).astype(jnp.int32)

    def greet(sem, reach):
        for shift in (-reach, reach):
            @pl.when(inside(shift, 0))
            def _():
                pl.semaphore_signal(
                    sem, inc=1, device_id=(row + shift, col), device_id_type=MESH)

    def meet(sem, reach):
        pl.semaphore_wait(sem, rows_at(reach))

    welcome()

    def halo_copy(stage, k, a, b):
        return pltpu.make_async_remote_copy(
            src_ref=part(stage, 4), dst_ref=part(stage, 8 - k),
            send_sem=halo_send.at[stage, k], recv_sem=halo_recv.at[stage, 8 - k],
            device_id=(row + a, col + b), device_id_type=MESH)

    def halo_start(stage):
        for k, a, b in around:
            @pl.when(inside(a, b))
            def _():
                halo_copy(stage, k, a, b).start()

    def halo_wait(stage):
        for k, a, b in around:
            @pl.when(inside(a, b))
            def _():
                pltpu.make_async_copy(
                    part(stage, k), part(stage, k), halo_recv.at[stage, k]).wait()

    def halo_done(stage):
        for k, a, b in around:
            @pl.when(inside(a, b))
            def _():
                pltpu.make_async_copy(
                    part(stage, 4), part(stage, 4), halo_send.at[stage, k]).wait()

    lane = lax.broadcasted_iota(jnp.int32, (1, size), 1)

    def reduce_start(stage, products):
        line = jnp.zeros((1, size), f32)
        for i, product in enumerate(products):
            line = jnp.where(lane == i, jnp.sum(product, keepdims=True), line)
        dots[stage, me] = line
        others(lambda where: pltpu.make_async_remote_copy(
            src_ref=dots.at[stage, me], dst_ref=dots.at[stage, me],
            send_sem=dot_send.at[stage], recv_sem=dot_recv.at[stage],
            device_id=where, device_id_type=MESH).start())

    def all_bytes(stage, sem):
        most = dots.at[stage, pl.ds(0, n_dev - 1)]
        return pltpu.make_async_copy(most, most, sem.at[stage])

    def reduce_wait(stage, count):
        all_bytes(stage, dot_recv).wait()
        if n_dev <= UNROLL_LIMIT:
            lines = [dots[stage, d] for d in range(n_dev)]
            while len(lines) > 1:
                lines = [sum(lines[i:i + 2]) for i in range(0, len(lines), 2)]
            total = lines[0]
        else:
            total = lax.fori_loop(
                0, n_dev, lambda d, acc: acc + dots[stage, d], jnp.zeros((1, size), f32))
        return [jnp.broadcast_to(total[:, i:i + 1], (blocks, size)) for i in range(count)]

    def operate(source, own):
        for n in range(blocks):
            for s in range(slots):
                pieces[n:n + 1, s * size:(s + 1) * size] = source[
                    pl.ds(index[n * slots + s], 1), :]
        left = pieces[...].astype(jnp.bfloat16)
        out = []
        for n in range(0, blocks, 2):
            acc = jnp.zeros((blocks, 2 * size), f32)
            for s in range(0, slots, 2):
                right = jnp.concatenate([
                    jnp.concatenate([vals[n + d, s], vals[n + d, s + 1]], axis=1)
                    for d in range(2)], axis=0)
                acc = acc + lax.dot_general(
                    left[:, s * size:(s + 2) * size], right,
                    (((1,), (1,)), ((), ())), preferred_element_type=f32)
            out.append(acc[n:n + 1, :size])
            out.append(acc[n + 1:n + 2, size:])
        return scale[...] * own + jnp.concatenate(out, axis=0)

    reaches = greetings(n_row)
    for n in range(blocks):
        for s in range(slots):
            index[n * slots + s] = jnp.where(
                s < live_ref[0, 0, n], cols_ref[0, 0, s, n], 9 * blocks)
    load_rhs.wait()
    near = 1
    for reach in range(1, REACH + 1):
        near = near + rows_at(reach)
    pl.semaphore_wait(barrier, near * n_col - 1)
    halo_start(0)
    for i, reach in enumerate(reaches):
        greet(meet_sem.at[i], reach)
        if i + 1 < len(reaches):
            meet(meet_sem.at[i], reach)
    load_scale.wait()
    for copy in load_vals:
        copy.wait()
    halo_wait(0)
    own = pl.ds(4 * blocks, blocks)
    rhs = first[own, :]
    image = operate(first, rhs)
    later[0, own, :] = image
    if reaches:
        meet(meet_sem.at[len(reaches) - 1], reaches[-1])
    reduce_start(0, [rhs * rhs, rhs * image, image * image])
    halo_start(1)

    def tall(x):
        return jnp.concatenate([x] * 10, axis=0)

    columns = []
    gram = [[None] * ITERS for _ in range(ITERS)]
    factor = [[None] * ITERS for _ in range(ITERS)]
    inverse = [None] * ITERS
    forward = []
    for j in range(ITERS):
        all_bytes(j, dot_send).wait()
        halo_done(j)
        if j + 1 < ITERS:
            halo_wait(j + 1)
        if j == 0:
            self_dot, cross_dot, image_dot = reduce_wait(0, 3)
            norm = jnp.sqrt(self_dot)
            inv_norm = 1.0 / norm
            inv_self = 1.0 / self_dot
            proj = [cross_dot * inv_self]
            square = image_dot * inv_self
        else:
            got = reduce_wait(j, j + 2)
            proj, square = got[:j + 1], got[j + 1]
        total = proj[0] * proj[0]
        for h in proj[1:]:
            total = total + h * h
        height = jnp.sqrt(square - total)
        if j + 1 < ITERS:
            inv_height = 1.0 / height
            if j == 0:
                wide_norm = tall(inv_norm)
                basis[0] = first[...] * wide_norm
                w = later[0] * wide_norm
            else:
                w = later[j]
            for i in range(j + 1):
                w = w - tall(proj[i]) * basis[i]
            basis[j + 1] = w * tall(inv_height)
            here = [basis[i, own, :] for i in range(j + 2)]
            image = operate(basis.at[j + 1], here[-1])
            if j + 2 < ITERS:
                later[j + 1, own, :] = image
            reduce_start(j + 1, [v * image for v in here] + [image * image])
            if j + 2 < ITERS:
                halo_start(j + 2)
        columns.append(proj + [height])
        for i in range(j + 1):
            acc = columns[i][0] * columns[j][0]
            for m in range(1, i + 2):
                acc = acc + columns[i][m] * columns[j][m]
            gram[j][i] = acc
        for i in range(j + 1):
            acc = gram[j][i]
            for m in range(i):
                acc = acc - factor[j][m] * factor[i][m]
            if i == j:
                factor[j][j] = jnp.sqrt(acc)
                inverse[j] = 1.0 / factor[j][j]
            else:
                factor[j][i] = acc * inverse[i]
        acc = norm * columns[j][0]
        for m in range(j):
            acc = acc - factor[j][m] * forward[m]
        forward.append(acc * inverse[j])
    weights = [None] * ITERS
    for i in reversed(range(ITERS)):
        acc = forward[i]
        for m in range(i + 1, ITERS):
            acc = acc - factor[m][i] * weights[m]
        weights[i] = acc * inverse[i]
    result = weights[0] * basis[0, own, :]
    for i in range(1, ITERS):
        result = result + weights[i] * basis[i, own, :]
    field_ref[0, 0] = result
    down = lax.broadcasted_iota(jnp.int32, (blocks, size), 0)
    along = lax.broadcasted_iota(jnp.int32, (blocks, size), 1)
    hess = jnp.zeros((blocks, size), f32)
    for j in range(ITERS):
        for i in range(j + 2):
            hess = jnp.where((down == j) & (along == i), columns[j][i], hess)
    hess_ref[...] = hess[:ITERS, :ITERS + 1]


def greetings(n_row):
    reaches, reach = [], REACH
    while reach < n_row - 1:
        reaches.append(reach)
        reach *= 2
    return reaches


def write_out(field_ref, hess_ref, field_out, hess_out, sems):
    copies = [
        pltpu.make_async_copy(field_ref, field_out, sems.at[0]),
        pltpu.make_async_copy(hess_ref, hess_out, sems.at[1]),
    ]
    for copy in copies:
        copy.start()
    for copy in copies:
        copy.wait()


def on_device(right_side, block_values, block_columns, live_slots, row_scale):
    n_row, n_col = lax.axis_size("row"), lax.axis_size("col")
    blocks, slots, size = block_values.shape[2:5]
    f32 = jnp.float32
    result, hess = pl.pallas_call(
        functools.partial(kernel, n_row, n_col),
        out_shape=(
            pltpu.VMEM(right_side.shape, f32),
            pltpu.VMEM((ITERS, ITERS + 1), f32),
        ),
        in_specs=[pl.BlockSpec(memory_space=pltpu.SMEM)] * 2
        + [pl.BlockSpec(memory_space=pltpu.HBM)] * 3,
        out_specs=(pl.BlockSpec(memory_space=pltpu.VMEM),) * 2,
        scratch_shapes=[
            pltpu.VMEM((blocks, slots, size, size), jnp.bfloat16),
            pltpu.VMEM((blocks, size), f32),
            pltpu.VMEM((10 * blocks, size), f32),
            pltpu.VMEM((ITERS - 1, 10 * blocks, size), f32),
            pltpu.VMEM((ITERS, 10 * blocks, size), f32),
            pltpu.VMEM((ITERS, n_row * n_col, 1, size), f32),
            pltpu.VMEM((blocks, slots * size), f32),
            pltpu.SMEM((blocks * slots,), jnp.int32),
            pltpu.SemaphoreType.DMA((2,)),
            pltpu.SemaphoreType.DMA((blocks,)),
            pltpu.SemaphoreType.DMA((ITERS, 9)),
            pltpu.SemaphoreType.DMA((ITERS, 9)),
            pltpu.SemaphoreType.DMA((ITERS,)),
            pltpu.SemaphoreType.DMA((ITERS,)),
            pltpu.SemaphoreType.REGULAR((max(1, len(greetings(n_row))),)),
        ],
        compiler_params=pltpu.CompilerParams(
            collective_id=0, has_side_effects=True, vmem_limit_bytes=60 << 20),
    )(block_columns.swapaxes(2, 3), live_slots, *[
        pltpu.with_memory_space_constraint(x, pltpu.HBM)
        for x in (right_side, row_scale, block_values)])
    result, hess = pl.pallas_call(
        write_out,
        out_shape=(
            jax.ShapeDtypeStruct(right_side.shape, f32),
            jax.ShapeDtypeStruct((ITERS, ITERS + 1), f32),
        ),
        in_specs=[pl.BlockSpec(memory_space=pltpu.VMEM)] * 2,
        out_specs=[pl.BlockSpec(memory_space=pltpu.HBM)] * 2,
        scratch_shapes=[pltpu.SemaphoreType.DMA((2,))],
        compiler_params=pltpu.CompilerParams(vmem_limit_bytes=1 << 20),
    )(result, hess)
    return result, hess.T


def solution(mesh):
    return jax.shard_map(
        on_device,
        mesh=mesh,
        in_specs=(
            P("row", "col", None, None),
            P("row", "col", None, None, None, None),
            P("row", "col", None, None),
            P("row", "col", None),
            P("row", "col", None, None),
        ),
        out_specs=(P("row", "col", None, None), P()),
        check_vma=False,
    )
```
